32 devices in a mesh: det: 8 (over y, x, core), bm: 4 (over z).
Axes of the slice: x: 2, y: 2, z: 4, core: 2. Of those that a mesh axis runs over, the one named last changes fastest.
Arguments:
- sky_alm: bfloat16 [2, 3, 16, 128], P(None, None, 'det'), may hold values from -6 to 6
- beam_blm: bfloat16 [2, 3, 16, 128], P(None, None, 'bm'), may hold values from -2.5 to 2.5
- wigner: bfloat16 [32, 16, 16, 128], P('det', None, 'bm'), may hold values from -0.03125 to 0.03125
- theta_index: int32 [128, 256], P('det'), may hold values from 0 to 3
- phi_index: int32 [128, 256], P('det'), may hold values from 0 to 16383
- psi_index: int32 [128, 256], P('det'), may hold values from 0 to 31
Outputs:
- tod: float32 [128, 256], P('det', 'bm')
The draws below stay inside these ranges and needn't reach their ends.
All inputs are finite; a program needn't handle non-finite values.
Results may differ from the reference program's by a relative error of at most 0.0029.
Values may be sent and summed in bfloat16 or wider, within the bound.
A program may use at most 64 MiB of HBM per device.

```python
import math
import jax
import jax.numpy as jnp
from jax import lax

LBAND = 128
BEAM_M = 16
NR = 4
SAMP = 256
NPHI = 16384
NPSI = 32
MWIN = 16
CYCLES = 32
DETS = 128
N_DET = 8


def set_ends(drawn, own_key, least, top_value):
    spot = [jax.random.randint(jax.random.fold_in(own_key, axis), (), 0, length) for axis, length in enumerate(drawn.shape)]
    main_axis = drawn.shape.index(max(drawn.shape))
    beside = spot[:main_axis] + [(spot[main_axis] + 1) % drawn.shape[main_axis]] + spot[main_axis + 1:]
    return drawn.at[tuple(spot)].set(least).at[tuple(beside)].set(top_value)


def shard_levels(stream_key, shape, cuts, least, high):
    level, own = 1.0, jax.random.fold_in(stream_key, 6)
    for axis_at, parts in cuts:
        draws = jnp.exp(jax.random.uniform(jax.random.fold_in(own, axis_at), (parts,), jnp.float32, least / len(cuts), high / len(cuts)))
        level = level * jnp.repeat(draws, shape[axis_at] // parts).reshape([-1 if axis == axis_at else 1 for axis in range(len(shape))])
    return level


def bell_draw(rng, extent, deviation, bound, split=(), kind=jnp.bfloat16):
    drawn = deviation * jax.random.normal(rng, extent, jnp.float32)
    if split:
        drawn = drawn * shard_levels(rng, extent, split, -0.22, 0.18)
    return jnp.clip(drawn, -bound, bound).astype(kind)


def setup_inputs(seed: int = 0) -> dict:
    splits = jax.random.split(jax.random.key(seed), 7)
    sky_alm = bell_draw(splits[0], (2, 3, MWIN, LBAND), 1.0, 6.0, ((2, 8),))
    beam_blm = bell_draw(splits[1], (2, 3, BEAM_M, LBAND), 6 ** -0.5, 2.5, ((2, 4),))
    wigner = bell_draw(splits[2], (CYCLES, MWIN, BEAM_M, LBAND), (LBAND * MWIN * BEAM_M) ** -0.5, 0.03125, ((0, 8), (2, 4)))
    theta_index = set_ends(jax.random.randint(splits[3], (DETS, SAMP), 0, NR), jax.random.fold_in(splits[3], 1), 0, NR - 1).astype(jnp.int32)
    phi_index = set_ends(jax.random.randint(splits[4], (DETS, SAMP), 0, NPHI), jax.random.fold_in(splits[4], 1), 0, NPHI - 1).astype(jnp.int32)
    psi_index = set_ends(jax.random.randint(splits[5], (DETS, SAMP), 0, NPSI), jax.random.fold_in(splits[5], 1), 0, NPSI - 1).astype(jnp.int32)
    return dict(sky_alm=sky_alm, beam_blm=beam_blm, wigner=wigner, theta_index=theta_index, phi_index=phi_index, psi_index=psi_index)


TWO_PI = 2.0 * math.pi


def spectra_of(sky, beam):
    sky_full = sky.astype(jnp.float32)[:, :, :, None, :]
    beam_full = beam.astype(jnp.float32)[:, :, None, :, :]
    real_part = jnp.sum(sky_full[0] * beam_full[0] - sky_full[1] * beam_full[1], axis=0)
    imag_part = jnp.sum(sky_full[0] * beam_full[1] + sky_full[1] * beam_full[0], axis=0)
    return jnp.stack([real_part, imag_part]).astype(jnp.bfloat16)


def product_first(left, right):
    dims = (((0,), (0,)), ((), ()))
    return lax.dot_general(left, right, dims, precision=lax.Precision.HIGHEST, preferred_element_type=jnp.float32)


def sample_tod(cube, theta, phi, psi, first_plane):
    cycles = cube.shape[1]
    planes = cube.shape[2]
    modes = cube.shape[3]
    plane_ids = first_plane + jnp.arange(planes, dtype=jnp.int32)
    psi_angle = TWO_PI * ((plane_ids[:, None] * psi[None, :]) % NPSI).astype(jnp.float32) / NPSI
    select = (theta[None, :] == jnp.arange(cycles, dtype=jnp.int32)[:, None]).astype(jnp.float32)
    cos_feat = (select[:, None, :] * jnp.cos(psi_angle)[None]).reshape(cycles * planes, -1)
    sin_feat = (select[:, None, :] * jnp.sin(psi_angle)[None]).reshape(cycles * planes, -1)
    flat = cube.reshape(2, cycles * planes, modes)
    k_real = product_first(flat[0], cos_feat) - product_first(flat[1], sin_feat)
    k_imag = product_first(flat[1], cos_feat) + product_first(flat[0], sin_feat)
    mode_ids = jnp.arange(modes, dtype=jnp.int32)
    phi_angle = TWO_PI * ((mode_ids[:, None] * phi[None, :]) % NPHI).astype(jnp.float32) / NPHI
    return jnp.sum(k_real * jnp.cos(phi_angle) - k_imag * jnp.sin(phi_angle), axis=0)


def reference(sky_alm, beam_blm, wigner, theta_index, phi_index, psi_index):
    spectra = lax.optimization_barrier(spectra_of(sky_alm, beam_blm)).astype(jnp.float32)
    tables = wigner.reshape(N_DET, NR, MWIN, BEAM_M, LBAND)

    def one_group(inputs):
        table, theta, phi, psi = inputs
        cube = jnp.einsum("rmpl,kmpl->krpm", table.astype(jnp.float32), spectra, precision=lax.Precision.HIGHEST)
        return sample_tod(cube, theta, phi, psi, 0)

    tod = lax.map(one_group, (tables, theta_index.reshape(N_DET, -1), phi_index.reshape(N_DET, -1), psi_index.reshape(N_DET, -1)))
    return tod.reshape(DETS, SAMP)
```

```python
import functools
import math

import jax
import jax.numpy as jnp
from jax import lax
from jax.experimental import pallas as pl
from jax.experimental.pallas import tpu as pltpu
from jax.sharding import PartitionSpec as P

NPHI = 16384
NPSI = 32

TWO_PI = 2.0 * math.pi
LANES = 128
ROWS = 8
F32 = jnp.float32
BF16 = jnp.bfloat16
MESH = pl.DeviceIdType.MESH


def cos_on_grid(step, grid):
    shift = (grid // 4).bit_length() - 1
    turn = (step + grid // 8) >> shift
    x = (step - (turn << shift)).astype(F32) * (TWO_PI / grid)
    x2 = x * x
    c = 1.0 + x2 * (-0.5 + x2 * (1 / 24 + x2 * (-1 / 720 + x2 * (1 / 40320))))
    s = x * (1.0 + x2 * (-1 / 6 + x2 * (1 / 120 + x2 * (-1 / 5040 + x2 * (1 / 362880)))))
    odd = (turn & 1) == 1
    value = jnp.where(odd, -s, c)
    return jnp.where((turn & 2) == 2, -value, value)


def partner(me, flip, n):
    out, bit = 0, 1
    while bit < n:
        digit = (me // bit) % 2
        out = out + bit * ((1 - digit) if flip & bit else digit)
        bit *= 2
    return out


def rows_of(values, groups, width):
    return jnp.concatenate([values[j * ROWS : (j + 1) * ROWS] for j in range(groups)], axis=1)


def kernel(
    n_det, n_bm,
    sky_hbm, beam_hbm, wig_hbm, theta_hbm, phi_hbm, psi_hbm, out_ref,
    sky_all, beam, wig, index, wide, feat, phase, cube_all,
    local_sem, sky_send, sky_recv, cube_send, cube_recv,
):
    det = lax.axis_index("det")
    bm = lax.axis_index("bm")
    local = [
        pltpu.make_async_copy(sky_hbm, sky_all.at[det], local_sem.at[0]),
        pltpu.make_async_copy(beam_hbm, beam, local_sem.at[1]),
        pltpu.make_async_copy(wig_hbm, wig, local_sem.at[2]),
        pltpu.make_async_copy(theta_hbm, index.at[0], local_sem.at[3]),
        pltpu.make_async_copy(phi_hbm, index.at[1], local_sem.at[4]),
        pltpu.make_async_copy(psi_hbm, index.at[2], local_sem.at[5]),
    ]
    for copy in local:
        copy.start()
    barrier = pltpu.get_barrier_semaphore()
    for flip in range(1, n_det):
        pl.semaphore_signal(
            barrier, inc=1, device_id=(partner(det, flip, n_det), bm), device_id_type=MESH
        )
    for step in range(1, n_bm):
        pl.semaphore_signal(
            barrier, inc=1, device_id=(det, (bm + step) % n_bm), device_id_type=MESH
        )
    local[0].wait()
    pl.semaphore_wait(barrier, n_det - 1 + n_bm - 1)
    sends = []
    for flip in range(n_det - 1, 0, -1):
        copy = pltpu.make_async_remote_copy(
            src_ref=sky_all.at[det],
            dst_ref=sky_all.at[det],
            send_sem=sky_send.at[flip],
            recv_sem=sky_recv.at[flip],
            device_id=(partner(det, flip, n_det), bm),
            device_id_type=MESH,
        )
        copy.start()
        sends.append(copy)
    for copy in local[1:]:
        copy.wait()

    cycles, flat, band = wig.shape
    planes = beam.shape[2]
    modes = flat // planes
    owned = sky_all.shape[3]
    pairs = cycles * planes
    depth = 2 * pairs
    per_tile = LANES // (2 * depth)
    tile_modes = per_tile * ROWS
    tiles = modes // tile_modes
    dets, samples = index.shape[1:]
    width = samples // n_bm
    groups = dets // ROWS

    for g in range(cycles):
        wide[g] = wig[g].astype(F32)

    def mine(values):
        own = values[:, :width]
        for i in range(1, n_bm):
            own = jnp.where(bm == i, values[:, i * width : (i + 1) * width], own)
        return rows_of(own, groups, width)

    theta, phi, psi = mine(index[0]), mine(index[1]), mine(index[2])
    span = groups * width
    k_rows = n_bm * depth
    row = lax.broadcasted_iota(jnp.int32, (k_rows, span), 0)
    plane = ((bm + row // depth) % n_bm) * planes + row % planes
    cycle = (row // planes) % cycles
    quarter = ((row // pairs) % 2) * (3 * NPSI // 4)
    m_rows = 2 * modes
    mrow = lax.broadcasted_iota(jnp.int32, (m_rows, span), 0)
    mode = (mrow // (2 * tile_modes)) * tile_modes + mrow % tile_modes
    mquarter = ((mrow // tile_modes) % 2) * (NPHI // 4)
    for j in range(ROWS):
        at = pl.ds(j * span, span)
        step = (plane * psi[j : j + 1] + quarter) & (NPSI - 1)
        value = jnp.where(cycle == theta[j : j + 1], cos_on_grid(step, NPSI), 0.0)
        high = value.astype(BF16)
        feat[:k_rows, at] = high
        feat[k_rows:, at] = (value - high.astype(F32)).astype(BF16)
        step = (mode * phi[j : j + 1] + mquarter) & (NPHI - 1)
        phase[:, at] = cos_on_grid(step, NPHI)

    for copy in sends:
        copy.wait_recv()

    lane = lax.broadcasted_iota(jnp.int32, (ROWS, LANES), 1)
    imag_row = (lane // (depth * per_tile)) % 2
    sin_column = (lane // pairs) % 2
    part = (imag_row + sin_column) % 2
    code = ((lane // depth) % per_tile * 2 + part) * pairs + lane % pairs
    sign = jnp.where((imag_row == 0) & (sin_column == 1), -1.0, 1.0)
    slots = tile_modes // owned
    for t in range(tiles):
        sky = [
            [
                sky_all[t * slots : (t + 1) * slots, r, c].astype(F32).reshape(tile_modes, band)
                for c in range(3)
            ]
            for r in range(2)
        ]
        packed = jnp.zeros((ROWS, LANES), F32)
        for h in range(per_tile):
            for p in range(planes):
                re = im = 0.0
                for c in range(3):
                    s0 = sky[0][c][h * ROWS : (h + 1) * ROWS]
                    s1 = sky[1][c][h * ROWS : (h + 1) * ROWS]
                    b0 = beam[0, c, p : p + 1].astype(F32)
                    b1 = beam[1, c, p : p + 1].astype(F32)
                    re = re + (s0 * b0 - s1 * b1)
                    im = im + (s0 * b1 + s1 * b0)
                re = re.astype(BF16).astype(F32)
                im = im.astype(BF16).astype(F32)
                first = (t * tile_modes + h * ROWS) * planes + p
                for g in range(cycles):
                    w = wide[g, pl.ds(first, ROWS, stride=planes)]
                    for k, spectra in enumerate((re, im)):
                        total = jnp.sum(w * spectra, axis=1, keepdims=True)
                        where = (h * 2 + k) * pairs + g * planes + p
                        packed = jnp.where(code == where, total, packed)
        cube_all[0, t] = packed * sign

    later = []
    for step in range(1, n_bm):
        copy = pltpu.make_async_remote_copy(
            src_ref=cube_all.at[0],
            dst_ref=cube_all.at[n_bm - step],
            send_sem=cube_send.at[n_bm - step],
            recv_sem=cube_recv.at[n_bm - step],
            device_id=(det, (bm + step) % n_bm),
            device_id_type=MESH,
        )
        copy.start()
        later.append(copy)
    for copy in later:
        copy.wait_recv()

    blocks = []
    for t in range(tiles):
        parts = [cube_all[s, t] for s in range(n_bm)]
        for q in range(2 * per_tile):
            blocks.append(
                jnp.concatenate([x[:, q * depth : (q + 1) * depth] for x in parts], axis=1)
            )
    left = jnp.concatenate(blocks, axis=0)
    high = left.astype(BF16)
    low = (left - high.astype(F32)).astype(BF16)
    both = jnp.concatenate(
        [jnp.concatenate([high, high], axis=1), jnp.concatenate([low, low], axis=1)], axis=0
    )
    for j in range(ROWS):
        at = pl.ds(j * span, span)
        y = jnp.dot(both, feat[:, at], preferred_element_type=F32)
        z = (y[:m_rows] + y[m_rows:]) * phase[:, at]
        total = jnp.sum(z, axis=0, keepdims=True)
        for i in range(groups):
            out_ref[pl.ds(i * ROWS + j, 1), :] = total[:, i * width : (i + 1) * width]

    for copy in sends + later:
        copy.wait_send()


def on_device(sky_alm, beam_blm, wigner, theta_index, phi_index, psi_index):
    n_det, n_bm = lax.axis_size("det"), lax.axis_size("bm")
    cycles, modes, planes, band = wigner.shape
    dets, samples = theta_index.shape
    width = samples // n_bm
    span = dets // ROWS * width
    depth = 2 * cycles * planes
    tiles = modes * 2 * depth // (ROWS * LANES)
    any_space = pl.BlockSpec(memory_space=pl.ANY)
    out = pl.pallas_call(
        functools.partial(kernel, n_det, n_bm),
        out_shape=jax.ShapeDtypeStruct((dets, width), F32),
        in_specs=[any_space] * 6,
        out_specs=pl.BlockSpec(memory_space=pltpu.VMEM),
        scratch_shapes=[
            pltpu.VMEM((n_det, *sky_alm.shape), BF16),
            pltpu.VMEM(beam_blm.shape, BF16),
            pltpu.VMEM((cycles, modes * planes, band), BF16),
            pltpu.VMEM((3, dets, samples), jnp.int32),
            pltpu.VMEM((cycles, modes * planes, band), F32),
            pltpu.VMEM((2 * n_bm * depth, ROWS * span), BF16),
            pltpu.VMEM((2 * modes, ROWS * span), F32),
            pltpu.VMEM((n_bm, tiles, ROWS, LANES), F32),
            pltpu.SemaphoreType.DMA((6,)),
            pltpu.SemaphoreType.DMA((n_det,)),
            pltpu.SemaphoreType.DMA((n_det,)),
            pltpu.SemaphoreType.DMA((n_bm,)),
            pltpu.SemaphoreType.DMA((n_bm,)),
        ],
        compiler_params=pltpu.CompilerParams(collective_id=0, has_side_effects=True),
    )(
        sky_alm,
        beam_blm,
        wigner.reshape(cycles, modes * planes, band),
        theta_index,
        phi_index,
        psi_index,
    )
    return out


def solution(mesh):
    placed = (
        P(None, None, "det", None),
        P(None, None, "bm", None),
        P("det", None, "bm", None),
        P("det", None),
        P("det", None),
        P("det", None),
    )
    return jax.shard_map(
        on_device, mesh=mesh, in_specs=placed, out_specs=P("det", "bm"), check_vma=False
    )
```

```python
import functools
import math

import jax
import jax.numpy as jnp
from jax import lax
from jax.experimental import pallas as pl
from jax.experimental.pallas import tpu as pltpu
from jax.sharding import PartitionSpec as P

NPHI = 16384
NPSI = 32

TWO_PI = 2.0 * math.pi
LANES = 128
ROWS = 8
F32 = jnp.float32
BF16 = jnp.bfloat16
MESH = pl.DeviceIdType.MESH


def cos_on_grid(step, grid):
    shift = (grid // 4).bit_length() - 1
    turn = (step + grid // 8) >> shift
    x = (step - (turn << shift)).astype(F32) * (TWO_PI / grid)
    x2 = x * x
    c = 1.0 + x2 * (-0.5 + x2 * (1 / 24 + x2 * (-1 / 720 + x2 * (1 / 40320))))
    s = x * (1.0 + x2 * (-1 / 6 + x2 * (1 / 120 + x2 * (-1 / 5040 + x2 * (1 / 362880)))))
    odd = (turn & 1) == 1
    value = jnp.where(odd, -s, c)
    return jnp.where((turn & 2) == 2, -value, value)


def partner(me, flip, n):
    out, bit = 0, 1
    while bit < n:
        digit = (me // bit) % 2
        out = out + bit * ((1 - digit) if flip & bit else digit)
        bit *= 2
    return out


def rows_of(values, groups, width):
    return jnp.concatenate([values[j * ROWS : (j + 1) * ROWS] for j in range(groups)], axis=1)


def kernel(
    n_det, n_bm,
    sky_hbm, beam_hbm, wig_hbm, theta_hbm, phi_hbm, psi_hbm, out_ref,
    sky_all, beam, wig, index, wide, feat, phase, cube_all,
    local_sem, sky_send, sky_recv, cube_send, cube_recv, ready,
):
    det = lax.axis_index("det")
    bm = lax.axis_index("bm")
    local = [
        pltpu.make_async_copy(sky_hbm, sky_all.at[det], local_sem.at[0]),
        pltpu.make_async_copy(beam_hbm, beam, local_sem.at[1]),
        pltpu.make_async_copy(wig_hbm, wig, local_sem.at[2]),
        pltpu.make_async_copy(theta_hbm, index.at[0], local_sem.at[3]),
        pltpu.make_async_copy(phi_hbm, index.at[1], local_sem.at[4]),
        pltpu.make_async_copy(psi_hbm, index.at[2], local_sem.at[5]),
    ]
    for copy in local:
        copy.start()
    barrier = pltpu.get_barrier_semaphore()
    for flip in range(1, n_det):
        pl.semaphore_signal(
            barrier, inc=1, device_id=(partner(det, flip, n_det), bm), device_id_type=MESH
        )
    relayed = n_bm == 4
    greeted = (1, 2) if relayed else range(1, n_bm)
    for flip in greeted:
        pl.semaphore_signal(
            barrier, inc=1, device_id=(det, partner(bm, flip, n_bm)), device_id_type=MESH
        )
    local[0].wait()
    pl.semaphore_wait(barrier, n_det - 1 + len(greeted))
    sends = []
    for flip in range(n_det - 1, 0, -1):
        copy = pltpu.make_async_remote_copy(
            src_ref=sky_all.at[det],
            dst_ref=sky_all.at[det],
            send_sem=sky_send.at[flip],
            recv_sem=sky_recv.at[flip],
            device_id=(partner(det, flip, n_det), bm),
            device_id_type=MESH,
        )
        copy.start()
        sends.append(copy)
    if relayed:
        pl.semaphore_signal(
            ready, inc=1, device_id=(det, partner(bm, 1, n_bm)), device_id_type=MESH
        )
    for copy in local[1:]:
        copy.wait()

    cycles, flat, band = wig.shape
    planes = beam.shape[2]
    modes = flat // planes
    owned = sky_all.shape[3]
    pairs = cycles * planes
    depth = 2 * pairs
    per_tile = LANES // (2 * depth)
    tile_modes = per_tile * ROWS
    tiles = modes // tile_modes
    dets, samples = index.shape[1:]
    width = samples // n_bm
    groups = dets // ROWS

    for g in range(cycles):
        wide[g] = wig[g].astype(F32)

    def mine(values):
        own = values[:, :width]
        for i in range(1, n_bm):
            own = jnp.where(bm == i, values[:, i * width : (i + 1) * width], own)
        return rows_of(own, groups, width)

    theta, phi, psi = mine(index[0]), mine(index[1]), mine(index[2])
    span = groups * width
    k_rows = n_bm * depth
    row = lax.broadcasted_iota(jnp.int32, (k_rows, span), 0)
    source = 0
    for flip in range(n_bm):
        source = jnp.where(row // depth == flip, partner(bm, flip, n_bm), source)
    plane = source * planes + row % planes
    cycle = (row // planes) % cycles
    quarter = ((row // pairs) % 2) * (3 * NPSI // 4)
    m_rows = 2 * modes
    mrow = lax.broadcasted_iota(jnp.int32, (m_rows, span), 0)
    mode = (mrow // (2 * tile_modes)) * tile_modes + mrow % tile_modes
    mquarter = ((mrow // tile_modes) % 2) * (NPHI // 4)
    for j in range(ROWS):
        at = pl.ds(j * span, span)
        step = (plane * psi[j : j + 1] + quarter) & (NPSI - 1)
        value = jnp.where(cycle == theta[j : j + 1], cos_on_grid(step, NPSI), 0.0)
        high = value.astype(BF16)
        feat[:k_rows, at] = high
        feat[k_rows:, at] = (value - high.astype(F32)).astype(BF16)
        step = (mode * phi[j : j + 1] + mquarter) & (NPHI - 1)
        phase[:, at] = cos_on_grid(step, NPHI)

    for copy in sends:
        copy.wait_recv()

    lane = lax.broadcasted_iota(jnp.int32, (ROWS, LANES), 1)
    imag_row = (lane // (depth * per_tile)) % 2
    sin_column = (lane // pairs) % 2
    part = (imag_row + sin_column) % 2
    code = ((lane // depth) % per_tile * 2 + part) * pairs + lane % pairs
    sign = jnp.where((imag_row == 0) & (sin_column == 1), -1.0, 1.0)
    slots = tile_modes // owned
    for t in range(tiles):
        sky = [
            [
                sky_all[t * slots : (t + 1) * slots, r, c].astype(F32).reshape(tile_modes, band)
                for c in range(3)
            ]
            for r in range(2)
        ]
        packed = jnp.zeros((ROWS, LANES), F32)
        for h in range(per_tile):
            for p in range(planes):
                re = im = 0.0
                for c in range(3):
                    s0 = sky[0][c][h * ROWS : (h + 1) * ROWS]
                    s1 = sky[1][c][h * ROWS : (h + 1) * ROWS]
                    b0 = beam[0, c, p : p + 1].astype(F32)
                    b1 = beam[1, c, p : p + 1].astype(F32)
                    re = re + (s0 * b0 - s1 * b1)
                    im = im + (s0 * b1 + s1 * b0)
                re = re.astype(BF16).astype(F32)
                im = im.astype(BF16).astype(F32)
                first = (t * tile_modes + h * ROWS) * planes + p
                for g in range(cycles):
                    w = wide[g, pl.ds(first, ROWS, stride=planes)]
                    for k, spectra in enumerate((re, im)):
                        total = jnp.sum(w * spectra, axis=1, keepdims=True)
                        where = (h * 2 + k) * pairs + g * planes + p
                        packed = jnp.where(code == where, total, packed)
        cube_all[0, t] = packed * sign

    later = []
    if relayed:
        pl.semaphore_wait(ready, 1)
    for flip in range(n_bm - 1, 0, -1):
        copy = pltpu.make_async_remote_copy(
            src_ref=cube_all.at[0],
            dst_ref=cube_all.at[flip],
            send_sem=cube_send.at[flip],
            recv_sem=cube_recv.at[flip],
            device_id=(det, partner(bm, flip, n_bm)),
            device_id_type=MESH,
        )
        copy.start()
        later.append(copy)
    for copy in later:
        copy.wait_recv()

    blocks = []
    for t in range(tiles):
        parts = [cube_all[s, t] for s in range(n_bm)]
        for q in range(2 * per_tile):
            blocks.append(
                jnp.concatenate([x[:, q * depth : (q + 1) * depth] for x in parts], axis=1)
            )
    left = jnp.concatenate(blocks, axis=0)
    high = left.astype(BF16)
    low = (left - high.astype(F32)).astype(BF16)
    both = jnp.concatenate(
        [jnp.concatenate([high, high], axis=1), jnp.concatenate([low, low], axis=1)], axis=0
    )
    y = jnp.dot(both, feat[...], preferred_element_type=F32)
    z = (y[:m_rows] + y[m_rows:]) * phase[...]
    total = jnp.sum(z, axis=0, keepdims=True)
    for j in range(ROWS):
        for i in range(groups):
            at = j * span + i * width
            out_ref[pl.ds(i * ROWS + j, 1), :] = total[:, at : at + width]

    for copy in sends + later:
        copy.wait_send()


def on_device(sky_alm, beam_blm, wigner, theta_index, phi_index, psi_index):
    n_det, n_bm = lax.axis_size("det"), lax.axis_size("bm")
    cycles, modes, planes, band = wigner.shape
    dets, samples = theta_index.shape
    width = samples // n_bm
    span = dets // ROWS * width
    depth = 2 * cycles * planes
    tiles = modes * 2 * depth // (ROWS * LANES)
    any_space = pl.BlockSpec(memory_space=pl.ANY)
    out = pl.pallas_call(
        functools.partial(kernel, n_det, n_bm),
        out_shape=pltpu.VMEM((dets, width), F32),
        in_specs=[any_space] * 6,
        out_specs=pl.BlockSpec(memory_space=pltpu.VMEM),
        scratch_shapes=[
            pltpu.VMEM((n_det, *sky_alm.shape), BF16),
            pltpu.VMEM(beam_blm.shape, BF16),
            pltpu.VMEM((cycles, modes * planes, band), BF16),
            pltpu.VMEM((3, dets, samples), jnp.int32),
            pltpu.VMEM((cycles, modes * planes, band), F32),
            pltpu.VMEM((2 * n_bm * depth, ROWS * span), BF16),
            pltpu.VMEM((2 * modes, ROWS * span), F32),
            pltpu.VMEM((n_bm, tiles, ROWS, LANES), F32),
            pltpu.SemaphoreType.DMA((6,)),
            pltpu.SemaphoreType.DMA((n_det,)),
            pltpu.SemaphoreType.DMA((n_det,)),
            pltpu.SemaphoreType.DMA((n_bm,)),
            pltpu.SemaphoreType.DMA((n_bm,)),
            pltpu.SemaphoreType.REGULAR,
        ],
        compiler_params=pltpu.CompilerParams(collective_id=0, has_side_effects=True),
    )(
        sky_alm,
        beam_blm,
        wigner.reshape(cycles, modes * planes, band),
        theta_index,
        phi_index,
        psi_index,
    )
    return out


def solution(mesh):
    placed = (
        P(None, None, "det", None),
        P(None, None, "bm", None),
        P("det", None, "bm", None),
        P("det", None),
        P("det", None),
        P("det", None),
    )
    return jax.shard_map(
        on_device, mesh=mesh, in_specs=placed, out_specs=P("det", "bm"), check_vma=False
    )
```

```python
import functools
import math

import jax
import jax.numpy as jnp
from jax import lax
from jax.experimental import pallas as pl
from jax.experimental.pallas import tpu as pltpu
from jax.sharding import PartitionSpec as P

NPHI = 16384
NPSI = 32

TWO_PI = 2.0 * math.pi
LANES = 128
ROWS = 8
F32 = jnp.float32
BF16 = jnp.bfloat16
MESH = pl.DeviceIdType.MESH


def cos_on_grid(step, grid):
    shift = (grid // 4).bit_length() - 1
    turn = (step + grid // 8) >> shift
    x = (step - (turn << shift)).astype(F32) * (TWO_PI / grid)
    x2 = x * x
    c = 1.0 + x2 * (-0.5 + x2 * (1 / 24 + x2 * (-1 / 720 + x2 * (1 / 40320))))
    s = x * (1.0 + x2 * (-1 / 6 + x2 * (1 / 120 + x2 * (-1 / 5040 + x2 * (1 / 362880)))))
    odd = (turn & 1) == 1
    value = jnp.where(odd, -s, c)
    return jnp.where((turn & 2) == 2, -value, value)


def partner(me, flip, n):
    out, bit = 0, 1
    while bit < n:
        digit = (me // bit) % 2
        out = out + bit * ((1 - digit) if flip & bit else digit)
        bit *= 2
    return out


def rows_of(values, groups, width):
    return jnp.concatenate([values[j * ROWS : (j + 1) * ROWS] for j in range(groups)], axis=1)


def kernel(
    n_det, n_bm,
    sky_hbm, beam_hbm, wig_hbm, theta_hbm, phi_hbm, psi_hbm, out_ref,
    sky_all, beam, wig, index, wide, feat, phase, cube_all,
    local_sem, sky_send, sky_recv, cube_send, cube_recv, ready,
):
    det = lax.axis_index("det")
    bm = lax.axis_index("bm")
    local = [
        pltpu.make_async_copy(sky_hbm, sky_all.at[det], local_sem.at[0]),
        pltpu.make_async_copy(beam_hbm, beam, local_sem.at[1]),
        pltpu.make_async_copy(wig_hbm, wig, local_sem.at[2]),
        pltpu.make_async_copy(theta_hbm, index.at[0], local_sem.at[3]),
        pltpu.make_async_copy(phi_hbm, index.at[1], local_sem.at[4]),
        pltpu.make_async_copy(psi_hbm, index.at[2], local_sem.at[5]),
    ]
    for copy in local:
        copy.start()
    barrier = pltpu.get_barrier_semaphore()
    for flip in range(1, n_det):
        pl.semaphore_signal(
            barrier, inc=1, device_id=(partner(det, flip, n_det), bm), device_id_type=MESH
        )
    relayed = n_bm == 4
    greeted = (1, 2) if relayed else range(1, n_bm)
    for flip in greeted:
        pl.semaphore_signal(
            barrier, inc=1, device_id=(det, partner(bm, flip, n_bm)), device_id_type=MESH
        )
    local[0].wait()
    pl.semaphore_wait(barrier, n_det - 1 + len(greeted))
    sends = []
    for flip in range(n_det - 1, 0, -1):
        copy = pltpu.make_async_remote_copy(
            src_ref=sky_all.at[det],
            dst_ref=sky_all.at[det],
            send_sem=sky_send.at[flip],
            recv_sem=sky_recv.at[flip],
            device_id=(partner(det, flip, n_det), bm),
            device_id_type=MESH,
        )
        copy.start()
        sends.append(copy)
    if relayed:
        pl.semaphore_signal(
            ready, inc=1, device_id=(det, partner(bm, 1, n_bm)), device_id_type=MESH
        )
    for copy in local[1:]:
        copy.wait()

    cycles, flat, band = wig.shape
    planes = beam.shape[2]
    modes = flat // planes
    owned = sky_all.shape[3]
    pairs = cycles * planes
    depth = 2 * pairs
    per_tile = LANES // (2 * depth)
    tile_modes = per_tile * ROWS
    tiles = modes // tile_modes
    dets, samples = index.shape[1:]
    width = samples // n_bm
    groups = dets // ROWS

    for g in range(cycles):
        wide[g] = wig[g].astype(F32)

    def mine(values):
        own = values[:, :width]
        for i in range(1, n_bm):
            own = jnp.where(bm == i, values[:, i * width : (i + 1) * width], own)
        return rows_of(own, groups, width)

    theta, phi, psi = mine(index[0]), mine(index[1]), mine(index[2])
    span = groups * width
    k_rows = n_bm * depth
    row = lax.broadcasted_iota(jnp.int32, (k_rows, span), 0)
    source = 0
    for flip in range(n_bm):
        source = jnp.where(row // depth == flip, partner(bm, flip, n_bm), source)
    plane = source * planes + row % planes
    cycle = (row // planes) % cycles
    quarter = ((row // pairs) % 2) * (3 * NPSI // 4)
    m_rows = 2 * modes
    mrow = lax.broadcasted_iota(jnp.int32, (m_rows, span), 0)
    mode = (mrow // (2 * tile_modes)) * tile_modes + mrow % tile_modes
    mquarter = ((mrow // tile_modes) % 2) * (NPHI // 4)
    for j in range(ROWS):
        at = pl.ds(j * span, span)
        step = (plane * psi[j : j + 1] + quarter) & (NPSI - 1)
        value = jnp.where(cycle == theta[j : j + 1], cos_on_grid(step, NPSI), 0.0)
        high = value.astype(BF16)
        feat[:k_rows, at] = high
        feat[k_rows:, at] = (value - high.astype(F32)).astype(BF16)
        step = (mode * phi[j : j + 1] + mquarter) & (NPHI - 1)
        phase[:, at] = cos_on_grid(step, NPHI)

    lane = lax.broadcasted_iota(jnp.int32, (ROWS, LANES), 1)
    imag_row = (lane // (depth * per_tile)) % 2
    sin_column = (lane // pairs) % 2
    part = (imag_row + sin_column) % 2
    code = ((lane // depth) % per_tile * 2 + part) * pairs + lane % pairs
    sign = jnp.where((imag_row == 0) & (sin_column == 1), -1.0, 1.0)
    slots = ROWS // owned
    halves = tiles == 1 and per_tile == 2 and slots * 2 == n_det and n_det & (n_det - 1) == 0
    arriving = sends[::-1]
    if not halves:
        for copy in arriving:
            copy.wait_recv()
    for t in range(tiles):
        packed = jnp.zeros((ROWS, LANES), F32)
        for turn in range(per_tile):
            h = turn
            if halves:
                h = (det // slots + turn) % 2
                for copy in arriving[slots - 1 :] if turn else arriving[: slots - 1]:
                    copy.wait_recv()
            block = t * per_tile + h
            sky = [
                [
                    sky_all[pl.ds(block * slots, slots), r, c].astype(F32).reshape(ROWS, band)
                    for c in range(3)
                ]
                for r in range(2)
            ]
            for p in range(planes):
                re = im = 0.0
                for c in range(3):
                    s0 = sky[0][c]
                    s1 = sky[1][c]
                    b0 = beam[0, c, p : p + 1].astype(F32)
                    b1 = beam[1, c, p : p + 1].astype(F32)
                    re = re + (s0 * b0 - s1 * b1)
                    im = im + (s0 * b1 + s1 * b0)
                re = re.astype(BF16).astype(F32)
                im = im.astype(BF16).astype(F32)
                first = block * (ROWS * planes) + p
                for g in range(cycles):
                    w = wide[g, pl.ds(first, ROWS, stride=planes)]
                    for k, spectra in enumerate((re, im)):
                        total = jnp.sum(w * spectra, axis=1, keepdims=True)
                        where = (h * 2 + k) * pairs + g * planes + p
                        packed = jnp.where(code == where, total, packed)
        cube_all[0, t] = packed * sign

    later = []
    if relayed:
        pl.semaphore_wait(ready, 1)
    for flip in range(n_bm - 1, 0, -1):
        copy = pltpu.make_async_remote_copy(
            src_ref=cube_all.at[0],
            dst_ref=cube_all.at[flip],
            send_sem=cube_send.at[flip],
            recv_sem=cube_recv.at[flip],
            device_id=(det, partner(bm, flip, n_bm)),
            device_id_type=MESH,
        )
        copy.start()
        later.append(copy)
    blocks = []
    for flip in range(n_bm):
        if flip:
            later[n_bm - 1 - flip].wait_recv()
        for t in range(tiles):
            x = cube_all[flip, t]
            for q in range(2 * per_tile):
                piece = x[:, q * depth : (q + 1) * depth]
                at = t * 2 * per_tile + q
                if flip:
                    blocks[at] = jnp.concatenate([blocks[at], piece], axis=1)
                else:
                    blocks.append(piece)
    left = jnp.concatenate(blocks, axis=0)
    high = left.astype(BF16)
    low = (left - high.astype(F32)).astype(BF16)
    both = jnp.concatenate(
        [jnp.concatenate([high, high], axis=1), jnp.concatenate([low, low], axis=1)], axis=0
    )
    y = jnp.dot(both, feat[...], preferred_element_type=F32)
    z = (y[:m_rows] + y[m_rows:]) * phase[...]
    total = jnp.sum(z, axis=0, keepdims=True)
    for j in range(ROWS):
        for i in range(groups):
            at = j * span + i * width
            out_ref[pl.ds(i * ROWS + j, 1), :] = total[:, at : at + width]

    for copy in sends + later:
        copy.wait_send()


def on_device(sky_alm, beam_blm, wigner, theta_index, phi_index, psi_index):
    n_det, n_bm = lax.axis_size("det"), lax.axis_size("bm")
    cycles, modes, planes, band = wigner.shape
    dets, samples = theta_index.shape
    width = samples // n_bm
    span = dets // ROWS * width
    depth = 2 * cycles * planes
    tiles = modes * 2 * depth // (ROWS * LANES)
    any_space = pl.BlockSpec(memory_space=pl.ANY)
    out = pl.pallas_call(
        functools.partial(kernel, n_det, n_bm),
        out_shape=pltpu.VMEM((dets, width), F32),
        in_specs=[any_space] * 6,
        out_specs=pl.BlockSpec(memory_space=pltpu.VMEM),
        scratch_shapes=[
            pltpu.VMEM((n_det, *sky_alm.shape), BF16),
            pltpu.VMEM(beam_blm.shape, BF16),
            pltpu.VMEM((cycles, modes * planes, band), BF16),
            pltpu.VMEM((3, dets, samples), jnp.int32),
            pltpu.VMEM((cycles, modes * planes, band), F32),
            pltpu.VMEM((2 * n_bm * depth, ROWS * span), BF16),
            pltpu.VMEM((2 * modes, ROWS * span), F32),
            pltpu.VMEM((n_bm, tiles, ROWS, LANES), F32),
            pltpu.SemaphoreType.DMA((6,)),
            pltpu.SemaphoreType.DMA((n_det,)),
            pltpu.SemaphoreType.DMA((n_det,)),
            pltpu.SemaphoreType.DMA((n_bm,)),
            pltpu.SemaphoreType.DMA((n_bm,)),
            pltpu.SemaphoreType.REGULAR,
        ],
        compiler_params=pltpu.CompilerParams(collective_id=0, has_side_effects=True),
    )(
        sky_alm,
        beam_blm,
        wigner.reshape(cycles, modes * planes, band),
        theta_index,
        phi_index,
        psi_index,
    )
    return out


def solution(mesh):
    placed = (
        P(None, None, "det", None),
        P(None, None, "bm", None),
        P("det", None, "bm", None),
        P("det", None),
        P("det", None),
        P("det", None),
    )
    return jax.shard_map(
        on_device, mesh=mesh, in_specs=placed, out_specs=P("det", "bm"), check_vma=False
    )
```
